32 devices in a mesh: blk: 16 (over z, y, core), rhs: 2 (over x).
Axes of the slice: x: 2, y: 2, z: 4, core: 2. Of those that a mesh axis runs over, the one named last changes fastest.
Arguments:
- signal: bfloat16 [131072, 256], P('blk', 'rhs'), may hold values from -6 to 6
- col_factor: bfloat16 [96, 131072], P(None, 'blk'), may hold values from -0.5 to 0.5
- row_factor: bfloat16 [96, 131072], P(None, 'blk'), may hold values from -0.625 to 0.625
- level_factor: bfloat16 [4, 16, 2, 64, 48, 192], P(None, 'blk', None, 'rhs'), may hold values from -0.4375 to 0.4375
- col_leaf_sizes: int32 [16, 128], P('blk'), may hold values from 1 to 128, 8192 in all within a row
- row_leaf_sizes: int32 [16, 128], P('blk'), may hold values from 1 to 128, 8192 in all within a row
- level_order: int32 [4, 16, 128], P(None, 'blk'), may hold values from 0 to 127, each once within a row
Outputs:
- result: bfloat16 [131072, 256], P('blk', 'rhs')
The draws below stay inside these ranges and needn't reach their ends.
Inputs may be any that keep to these rules, and one draw needn't show every extreme that they name: `col_leaf_sizes`: row d lists in order the sizes of the 128 column leaves that cover unknowns d * 8192 to (d + 1) * 8192 - 1; each row sums to 8192 and its largest entry is 128. `row_leaf_sizes`: row d lists in order the sizes of the 128 row leaves that cover unknowns d * 8192 to (d + 1) * 8192 - 1; each row sums to 8192 and its largest entry is 128. Every level_order[l, d, :] is a permutation of 0 to 127.
All inputs are finite; a program needn't handle non-finite values.
Results may differ from the reference program's by a relative error of at most 0.0076.
Values may be sent and summed in bfloat16 or wider, within the bound.
No kernel may reach another device: no remote copies, remote signals or barrier semaphores. Data moves between devices by JAX's collectives and lax.ppermute only.
A program may use at most 128 MiB of HBM per device.

```python
import math
import jax
import jax.numpy as jnp
import numpy as np
from jax import lax

K = 48
P_DEV = 8192
LEAVES_DEV = 128
LEAFMAX = 128
LEVELS = 4
COLS_DEV = 64
GROUPS = 16
R = 128
N = 131072
PEER_BLOCKS = 8


def block_levels(own_key, shape, split, least, high):
    def one(axis_at, parts):
        steps = jax.random.uniform(jax.random.fold_in(jax.random.fold_in(own_key, 6), axis_at), (parts,), jnp.float32, least / len(split), high / len(split))
        return jnp.repeat(jnp.exp(steps), shape[axis_at] // parts).reshape((-1,) + (1,) * (len(shape) - axis_at - 1))

    level = one(*split[0])
    for cut in split[1:]:
        level = level * one(*cut)
    return level


def length_profile(count, total, bound, slope):
    loads = [(1 << 20) // math.isqrt(standing ** slope) + 1 for standing in range(2, count + 1)]
    rest, holding = total - bound - (count - 1), [1] * (count - 1)
    while rest > 0:
        movable = [i for i in range(count - 1) if holding[i] < bound]
        whole, budget = sum([loads[i] for i in movable]), rest
        for i in movable:
            more = min(bound - holding[i], max(1, budget * loads[i] // whole), rest)
            holding[i] = holding[i] + more
            rest = rest - more
    return np.array([bound] + holding)


def uneven_parts(stream_key, number_of, total, bound, slope):
    if number_of == 2:
        one = jax.random.randint(stream_key, (), max(1, total - bound), min(bound, total - 1) + 1)
        return jnp.stack([one, total - one])
    tallies = jnp.asarray(length_profile(number_of, total, bound, slope), jnp.int32)
    twos = (number_of - 1) // 2
    giver, receiver = tallies[1:1 + 2 * twos:2], tallies[2:2 + 2 * twos:2]
    margin = jnp.minimum(giver - 1, bound - receiver)
    passed = jax.random.randint(jax.random.fold_in(stream_key, 1), (twos,), 0, 1 << 20) % (margin + 1)
    tallies = tallies.at[1:1 + 2 * twos:2].set(giver - passed).at[2:2 + 2 * twos:2].set(receiver + passed)
    return tallies[jax.random.permutation(jax.random.fold_in(stream_key, 2), number_of)]


def gaussian(key, extent, spread, limit, cuts=(), kind=jnp.bfloat16):
    loudness = block_levels(key, extent, cuts, -0.22, 0.18) if cuts else 1.0
    values = jax.random.normal(key, extent, jnp.float32) * spread * loudness
    return jnp.minimum(jnp.maximum(values, -limit), limit).astype(kind)


def setup_inputs(seed: int = 0) -> dict:
    seeds = jax.random.split(jax.random.key(seed), 8)
    return {
        "signal": gaussian(seeds[0], (N, 2 * R), 1.0, 6.0, ((0, 16), (1, 2))),
        "col_factor": gaussian(seeds[1], (2 * K, N), (2 * P_DEV // LEAVES_DEV) ** -0.5, 0.5, ((1, 16),)),
        "row_factor": gaussian(seeds[2], (2 * K, N), (2 * K) ** -0.5, 0.625, ((1, 16),)),
        "level_factor": gaussian(seeds[3], (LEVELS, GROUPS, 2, LEAVES_DEV // 2, K, 4 * K), (4 * K) ** -0.5, 0.4375, ((1, 16), (3, 2))),
        "col_leaf_sizes": jax.vmap(lambda own: uneven_parts(own, LEAVES_DEV, P_DEV, LEAFMAX, 1))(jax.random.split(seeds[4], GROUPS)).reshape((GROUPS, LEAVES_DEV)).astype(jnp.int32),
        "row_leaf_sizes": jax.vmap(lambda own: uneven_parts(own, LEAVES_DEV, P_DEV, LEAFMAX, 1))(jax.random.split(seeds[5], GROUPS)).reshape((GROUPS, LEAVES_DEV)).astype(jnp.int32),
        "level_order": jax.vmap(lambda own: jax.random.permutation(own, LEAVES_DEV))(jax.random.split(seeds[6], LEVELS * GROUPS)).reshape((LEVELS, GROUPS, LEAVES_DEV)).astype(jnp.int32),
    }


def turn_parts(values, groups):
    pieces = values.reshape(values.shape[:-1] + (groups, 2, values.shape[-1] // (2 * groups)))
    turned = jnp.stack([-pieces[..., 1, :], pieces[..., 0, :]], axis=-2)
    return turned.reshape(values.shape)


def leaf_windows(leaf_sizes):
    leaf_sizes = leaf_sizes.astype(jnp.int32)
    starts = (jnp.cumsum(leaf_sizes) - leaf_sizes).astype(jnp.int32)
    offsets = jnp.arange(LEAFMAX, dtype=jnp.int32)
    window_index = jnp.minimum(starts[:, None] + offsets[None, :], P_DEV - 1).astype(jnp.int32)
    inside = offsets[None, :] < leaf_sizes[:, None]
    return starts, window_index, inside


def leaf_coefficients(operands):
    points, factor, leaf_sizes = operands
    starts, window_index, inside = leaf_windows(leaf_sizes)
    flat_index = window_index.reshape(-1)
    gathered = jnp.take(points, flat_index, axis=0).reshape(LEAVES_DEV, LEAFMAX, points.shape[-1])
    weights = jnp.take(factor, flat_index, axis=1).reshape(2, K, LEAVES_DEV, LEAFMAX)
    weights = jnp.where(inside[None, None], weights, jnp.zeros_like(weights))
    paired = jnp.stack([gathered, turn_parts(gathered, R // COLS_DEV)])
    products = jnp.einsum("tkbi,tbic->bkc", weights.astype(jnp.float32), paired.astype(jnp.float32))
    return products.astype(jnp.bfloat16)


def mix_level(operands):
    arrived, weights = operands
    groups = R // COLS_DEV
    partner = jnp.roll(arrived, LEAVES_DEV // 2, axis=0)
    stacked = jnp.concatenate([arrived, turn_parts(arrived, groups), partner, turn_parts(partner, groups)], axis=1)
    products = jnp.einsum("bkm,bmc->bkc", weights.astype(jnp.float32), stacked.astype(jnp.float32))
    return products.astype(jnp.bfloat16)


def leaf_outputs(operands):
    coefficients, factor, leaf_sizes = operands
    starts, window_index, inside = leaf_windows(leaf_sizes)
    weights = jnp.take(factor, window_index.reshape(-1), axis=1).reshape(2, K, LEAVES_DEV, LEAFMAX)
    paired = jnp.stack([coefficients, turn_parts(coefficients, R // COLS_DEV)])
    leafwise = jnp.einsum("tkbi,tbkc->bic", weights.astype(jnp.float32), paired.astype(jnp.float32))
    points = jnp.arange(P_DEV, dtype=jnp.int32)
    covered = starts[None, :] <= points[:, None]
    leaf_index = (jnp.sum(covered.astype(jnp.int32), axis=1) - 1).astype(jnp.int32)
    leaf_start = jnp.max(jnp.where(covered, starts[None, :], jnp.zeros_like(starts)[None, :]), axis=1).astype(jnp.int32)
    flat_index = (leaf_index * LEAFMAX + points - leaf_start).astype(jnp.int32)
    return jnp.take(leafwise.reshape(-1, leafwise.shape[-1]), flat_index, axis=0).astype(jnp.bfloat16)


def reference(signal, col_factor, row_factor, level_factor, col_leaf_sizes, row_leaf_sizes, level_order):
    columns = signal.shape[-1]
    grouped = signal.reshape(GROUPS, P_DEV, columns)
    col_parts = col_factor.reshape(2 * K, GROUPS, P_DEV).transpose(1, 0, 2)
    coefficients = lax.map(leaf_coefficients, (grouped, col_parts, col_leaf_sizes))
    for layer_index in range(LEVELS):
        chosen = level_order[layer_index].astype(jnp.int32)[:, :, None, None]
        outgoing = jnp.take_along_axis(coefficients, chosen, axis=1)
        arrived = outgoing.reshape(GROUPS, GROUPS, PEER_BLOCKS, K, columns)
        arrived = arrived.transpose(1, 0, 2, 3, 4).reshape(GROUPS, LEAVES_DEV, K, columns)
        weights = level_factor[layer_index].reshape(GROUPS, LEAVES_DEV, K, 4 * K)
        coefficients = lax.map(mix_level, (arrived, weights))
    row_parts = row_factor.reshape(2 * K, GROUPS, P_DEV).transpose(1, 0, 2)
    outputs = lax.map(leaf_outputs, (coefficients, row_parts, row_leaf_sizes))
    return outputs.reshape(N, columns)
```

```python
import functools

import jax
import jax.numpy as jnp
from jax import lax
from jax.experimental import pallas as pl
from jax.experimental.pallas import tpu as pltpu
from jax.sharding import PartitionSpec as P

LEAFMAX = 128
TILE = 128
ROWS = 16


def turned(values):
    half = values.shape[-1] // 2
    return jnp.concatenate([-values[:, half:], values[:, :half]], axis=1)


def leaf_in_kernel(
    groups, me_ref, sizes_ref, order_ref, signal_hbm, factor_hbm, out_ref,
    signal, factor, starts, sem_signal, sem_factor,
):
    leaves, rank, columns = out_ref.shape
    points = signal.shape[0]
    copies = [
        pltpu.make_async_copy(signal_hbm, signal, sem_signal),
        pltpu.make_async_copy(factor_hbm, factor, sem_factor),
    ]
    for copy in copies:
        copy.start()
    peer_blocks = leaves // groups
    me = me_ref[0]

    def place(b, total):
        starts[b] = total
        return total + sizes_ref[b]

    lax.fori_loop(0, leaves, place, jnp.int32(0), unroll=8)
    for copy in copies:
        copy.wait()
    lane = lax.broadcasted_iota(jnp.int32, (ROWS, 2 * TILE), 1)

    def slot_body(slot, carry):
        group = (slot // peer_blocks) ^ me
        leaf = order_ref[group * peer_blocks + slot % peer_blocks]
        start = starts[leaf]
        chunk = jnp.minimum(start // TILE, points // TILE - 2)
        base = pl.multiple_of(chunk * TILE, TILE)
        low = start - base
        inside = (lane >= low) & (lane < low + sizes_ref[leaf])
        keep = jnp.where(inside, 1.0, 0.0).astype(jnp.bfloat16)
        weights = factor[:, pl.ds(base, 2 * TILE)]
        weights = weights.reshape(2 * rank // ROWS, ROWS, 2 * TILE) * keep[None]
        weights = weights.reshape(2 * rank, 2 * TILE)
        sums = jnp.dot(
            weights, signal[pl.ds(base, 2 * TILE), :], preferred_element_type=jnp.float32
        )
        out_ref[slot] = (sums[:rank] + turned(sums[rank:])).astype(out_ref.dtype)
        return carry

    lax.fori_loop(0, leaves, slot_body, 0, unroll=4)


def leaf_in(me, sizes, order, signal, factor, groups):
    points, columns = signal.shape
    leaves = sizes.shape[0]
    rank = factor.shape[0] // 2
    smem = pl.BlockSpec(memory_space=pltpu.SMEM)
    return pl.pallas_call(
        functools.partial(leaf_in_kernel, groups),
        out_shape=jax.ShapeDtypeStruct((leaves, rank, columns), jnp.bfloat16),
        in_specs=[smem, smem, smem]
        + [pl.BlockSpec(memory_space=pl.ANY)] * 2,
        out_specs=pl.BlockSpec(memory_space=pltpu.VMEM),
        scratch_shapes=[
            pltpu.VMEM(signal.shape, signal.dtype),
            pltpu.VMEM(factor.shape, factor.dtype),
            pltpu.SMEM((leaves,), jnp.int32),
            pltpu.SemaphoreType.DMA,
            pltpu.SemaphoreType.DMA,
        ],
        compiler_params=pltpu.CompilerParams(vmem_limit_bytes=16 * 2**20),
        name="leaf_in",
    )(me, sizes, order, signal, factor)


def mix_kernel(groups, parts, me_ref, slot_ref, *refs):
    blocks = refs[:groups]
    weights = refs[groups : groups + parts]
    out_ref = refs[groups + parts]
    peer_blocks, rank, columns = blocks[0].shape
    leaves = groups * peer_blocks
    pairs = leaves // 2
    per_part = pairs // parts
    me, part_me = me_ref[0], me_ref[1]

    def product(block, stacked):
        h, i = block // pairs, block % pairs
        source = (i // per_part) ^ part_me
        inner = i % per_part
        own = weights[0][0, h, inner]
        for k in range(1, parts):
            own = jnp.where(source == k, weights[k][0, h, inner], own)
        sums = jnp.dot(own, stacked, preferred_element_type=jnp.float32)
        out_ref[slot_ref[block]] = sums.astype(out_ref.dtype)

    for d in range(groups // 2):
        other = d + groups // 2

        def body(q, carry):
            first, second = blocks[d][q], blocks[other][q]
            both = jnp.concatenate([first, turned(first)], axis=0)
            also = jnp.concatenate([second, turned(second)], axis=0)
            product((me ^ d) * peer_blocks + q, jnp.concatenate([both, also], axis=0))
            product((me ^ other) * peer_blocks + q, jnp.concatenate([also, both], axis=0))
            return carry

        lax.fori_loop(0, peer_blocks, body, 0, unroll=min(4, peer_blocks))


def mix_level(me, slots, blocks, weights):
    groups, parts = len(blocks), len(weights)
    peer_blocks, rank, columns = blocks[0].shape
    smem = pl.BlockSpec(memory_space=pltpu.SMEM)
    vmem = pl.BlockSpec(memory_space=pltpu.VMEM)
    return pl.pallas_call(
        functools.partial(mix_kernel, groups, parts),
        out_shape=jax.ShapeDtypeStruct((groups * peer_blocks, rank, columns), jnp.bfloat16),
        in_specs=[smem, smem] + [vmem] * (groups + parts),
        out_specs=vmem,
        compiler_params=pltpu.CompilerParams(vmem_limit_bytes=24 * 2**20),
        name="mix_level",
    )(me, slots, *blocks, *weights)


def leaf_out_kernel(starts_ref, blocks, factor, out_hbm, out, sem):
    leaves, rank, columns = blocks.shape
    points = out_hbm.shape[0]
    row = lax.broadcasted_iota(jnp.int32, (ROWS, columns), 0)

    def body(leaf, carry):
        start = starts_ref[leaf]
        base = pl.multiple_of(start // ROWS * ROWS, ROWS)
        block = blocks[leaf]
        stacked = jnp.concatenate(
            [block, turned(block), jnp.zeros((TILE - 2 * rank, columns), block.dtype)], axis=0
        )
        sums = jnp.dot(
            factor[pl.ds(base, LEAFMAX + ROWS), :], stacked, preferred_element_type=jnp.float32
        )
        before = out[pl.ds(base, ROWS), :].astype(jnp.float32)
        head = jnp.where(row >= start - base, sums[:ROWS], before)
        out[pl.ds(base, ROWS), :] = head.astype(out.dtype)
        rest = pl.multiple_of(base + ROWS, ROWS)
        out[pl.ds(rest, LEAFMAX), :] = sums[ROWS:].astype(out.dtype)
        return carry

    lax.fori_loop(0, leaves, body, 0, unroll=4)
    copy = pltpu.make_async_copy(out.at[pl.ds(0, points)], out_hbm, sem)
    copy.start()
    copy.wait()


def leaf_out(starts, blocks, factor, points):
    columns = blocks.shape[-1]
    vmem = pl.BlockSpec(memory_space=pltpu.VMEM)
    return pl.pallas_call(
        leaf_out_kernel,
        out_shape=jax.ShapeDtypeStruct((points, columns), jnp.bfloat16),
        in_specs=[pl.BlockSpec(memory_space=pltpu.SMEM), vmem, vmem],
        out_specs=pl.BlockSpec(memory_space=pl.ANY),
        scratch_shapes=[
            pltpu.VMEM((points + LEAFMAX + ROWS, columns), jnp.bfloat16),
            pltpu.SemaphoreType.DMA,
        ],
        compiler_params=pltpu.CompilerParams(vmem_limit_bytes=16 * 2**20),
        name="leaf_out",
    )(starts, blocks, factor)


def local(
    groups, parts,
    signal, col_factor, row_factor, level_factor, col_leaf_sizes, row_leaf_sizes, level_order,
):
    levels, leaves = level_order.shape[0], level_order.shape[2]
    peer_blocks = leaves // groups
    index, part = lax.axis_index("blk"), lax.axis_index("rhs")
    me = jnp.stack([index, part]).astype(jnp.int32)
    order = level_order[:, 0]

    ids = lax.iota(jnp.int32, leaves)
    hit = order[:, None, :] == ids[None, :, None]
    place = jnp.sum(jnp.where(hit, ids[None, None, :], 0), axis=2)
    slots = ((place // peer_blocks) ^ index) * peer_blocks + place % peer_blocks
    row_sizes = row_leaf_sizes[0]
    row_starts = (jnp.cumsum(row_sizes) - row_sizes).astype(jnp.int32)
    turned_factor = jnp.pad(
        row_factor.T, ((0, LEAFMAX + ROWS), (0, TILE - row_factor.shape[0]))
    )

    weights = []
    for level in range(levels):
        own = level_factor[level]
        held = [own]
        for k in range(1, parts):
            held.append(lax.ppermute(own, "rhs", [(p, p ^ k) for p in range(parts)]))
        weights.append(held)

    outgoing = leaf_in(me, col_leaf_sizes[0], order[0], signal, col_factor, groups)
    for level in range(levels):
        arrived = []
        for d in range(groups):
            block = outgoing[d * peer_blocks : (d + 1) * peer_blocks]
            if d:
                block = lax.ppermute(block, "blk", [(g, g ^ d) for g in range(groups)])
            arrived.append(block)
        target = slots[level + 1] if level + 1 < levels else ids
        outgoing = mix_level(me, target, arrived, weights[level])
    return leaf_out(row_starts, outgoing, turned_factor, signal.shape[0])


def solution(mesh):
    in_specs = (
        P("blk", "rhs"),
        P(None, "blk"),
        P(None, "blk"),
        P(None, "blk", None, "rhs", None, None),
        P("blk", None),
        P("blk", None),
        P(None, "blk", None),
    )
    body = functools.partial(local, mesh.shape["blk"], mesh.shape["rhs"])
    return jax.shard_map(
        body, mesh=mesh, in_specs=in_specs, out_specs=P("blk", "rhs"), check_vma=False
    )
```

```python
import functools

import jax
import jax.numpy as jnp
from jax import lax
from jax.experimental import pallas as pl
from jax.experimental.pallas import tpu as pltpu
from jax.sharding import PartitionSpec as P

LEAFMAX = 128
TILE = 128
ROWS = 16

SMEM = pl.BlockSpec(memory_space=pltpu.SMEM)
VMEM = pl.BlockSpec(memory_space=pltpu.VMEM)
ANY = pl.BlockSpec(memory_space=pl.ANY)
HBM = pl.BlockSpec(memory_space=pltpu.HBM)


def cost(micros):
    return pl.CostEstimate(flops=micros * 10**7, bytes_accessed=0, transcendentals=0)


def sign_row(rows, columns):
    lane = lax.broadcasted_iota(jnp.int32, (rows, columns), 1)
    return jnp.where(lane < columns // 2, -1.0, 1.0)


def turned(values, sign):
    return pltpu.roll(values, values.shape[-1] // 2, 1) * sign


def place_starts(sizes_ref, starts_ref):
    def place(b, total):
        starts_ref[b] = total
        return total + sizes_ref[b]

    lax.fori_loop(0, sizes_ref.shape[0], place, jnp.int32(0), unroll=8)


def leaf_in_kernel(
    groups, me_ref, sizes_ref, order_ref, signal_hbm, factor_hbm, levels_hbm, *refs
):
    count = levels_hbm.shape[0]
    out_ref, level_refs = refs[0], refs[1 : 1 + count]
    starts, signal, factor, held, inward, arrive, leave = refs[1 + count :]
    inputs = [
        pltpu.make_async_copy(factor_hbm, factor, inward.at[0]),
        pltpu.make_async_copy(signal_hbm, signal, inward.at[1]),
    ]
    loads = [
        pltpu.make_async_copy(levels_hbm.at[k], held.at[k], arrive.at[k]) for k in range(count)
    ]
    stores = [
        pltpu.make_async_copy(held.at[k], level_refs[k], leave.at[k]) for k in range(count)
    ]
    for load in inputs + loads:
        load.start()
    leaves, rank, columns = out_ref.shape
    points = signal.shape[0]
    peer_blocks = leaves // groups
    me = me_ref[0]
    place_starts(sizes_ref, starts)
    for load in inputs:
        load.wait()
    lane = lax.broadcasted_iota(jnp.int32, (ROWS, 2 * TILE), 1)
    sign = sign_row(rank, columns)

    def body(slot, carry):
        group = (slot // peer_blocks) ^ me
        leaf = order_ref[group * peer_blocks + slot % peer_blocks]
        start = starts[leaf]
        chunk = jnp.minimum(start // TILE, points // TILE - 2)
        base = pl.multiple_of(chunk * TILE, TILE)
        low = start - base
        inside = (lane >= low) & (lane < low + sizes_ref[leaf])
        keep = jnp.where(inside, 1.0, 0.0).astype(jnp.bfloat16)
        weights = factor[:, pl.ds(base, 2 * TILE)]
        weights = weights.reshape(2 * rank // ROWS, ROWS, 2 * TILE) * keep[None]
        weights = weights.reshape(2 * rank, 2 * TILE)
        sums = jnp.dot(
            weights, signal[pl.ds(base, 2 * TILE), :], preferred_element_type=jnp.float32
        )
        out_ref[slot] = (sums[:rank] + turned(sums[rank:], sign)).astype(out_ref.dtype)
        return carry

    step = leaves // count
    for k in range(count):
        lax.fori_loop(k * step, (k + 1) * step, body, 0, unroll=32)
        loads[k].wait()
        stores[k].start()
    for store in stores:
        store.wait()


def leaf_in(me, sizes, order, signal, factor, level_factor, groups):
    points, columns = signal.shape
    leaves = sizes.shape[0]
    rank = factor.shape[0] // 2
    count = level_factor.shape[0]
    return pl.pallas_call(
        functools.partial(leaf_in_kernel, groups),
        out_shape=[jax.ShapeDtypeStruct((leaves, rank, columns), jnp.bfloat16)]
        + [jax.ShapeDtypeStruct(level_factor.shape[1:], level_factor.dtype)] * count,
        in_specs=[SMEM, SMEM, SMEM, HBM, HBM, HBM],
        out_specs=[VMEM] + [HBM] * count,
        scratch_shapes=[
            pltpu.SMEM((leaves,), jnp.int32),
            pltpu.VMEM(signal.shape, signal.dtype),
            pltpu.VMEM(factor.shape, factor.dtype),
            pltpu.VMEM(level_factor.shape, level_factor.dtype),
            pltpu.SemaphoreType.DMA((2,)),
            pltpu.SemaphoreType.DMA((count,)),
            pltpu.SemaphoreType.DMA((count,)),
        ],
        compiler_params=pltpu.CompilerParams(vmem_limit_bytes=50000 * 2**10),
        cost_estimate=cost(4),
        name="leaf_in",
    )(me, sizes, order, signal, factor, level_factor)


def flip_kernel(factor, out_ref):
    rows, points = factor.shape
    fill = jnp.zeros((TILE - rows, TILE), factor.dtype)

    def body(chunk, carry):
        base = pl.multiple_of(chunk * TILE, TILE)
        piece = jnp.concatenate([factor[:, pl.ds(base, TILE)], fill], axis=0)
        out_ref[pl.ds(base, TILE), :] = piece.T
        return carry

    lax.fori_loop(0, points // TILE, body, 0, unroll=4)
    tail = LEAFMAX + ROWS
    out_ref[pl.ds(points, tail), :] = jnp.zeros((tail, TILE), factor.dtype)


def flip(factor):
    rows, points = factor.shape
    return pl.pallas_call(
        flip_kernel,
        out_shape=jax.ShapeDtypeStruct((points + LEAFMAX + ROWS, TILE), factor.dtype),
        in_specs=[VMEM],
        out_specs=VMEM,
        compiler_params=pltpu.CompilerParams(vmem_limit_bytes=8 * 2**20),
        cost_estimate=cost(4),
        name="flip",
    )(factor)


def mix_kernel(groups, parts, me_ref, slot_ref, *refs):
    blocks = refs[:groups]
    weights = refs[groups : groups + parts]
    out_ref = refs[groups + parts]
    peer_blocks, rank, columns = blocks[0].shape
    leaves = groups * peer_blocks
    pairs = leaves // 2
    per_part = pairs // parts
    me, part_me = me_ref[0], me_ref[1]
    sign = sign_row(rank, columns).astype(jnp.bfloat16)

    def product(block, stacked):
        h, i = block // pairs, block % pairs
        source = (i // per_part) ^ part_me
        inner = i % per_part
        own = weights[0][0, h, inner]
        for k in range(1, parts):
            own = jnp.where(source == k, weights[k][0, h, inner], own)
        sums = jnp.dot(own, stacked, preferred_element_type=jnp.float32)
        out_ref[slot_ref[block]] = sums.astype(out_ref.dtype)

    for d in range(groups // 2):
        other = d + groups // 2

        def body(q, carry):
            first, second = blocks[d][q], blocks[other][q]
            both = jnp.concatenate([first, turned(first, sign)], axis=0)
            also = jnp.concatenate([second, turned(second, sign)], axis=0)
            product((me ^ d) * peer_blocks + q, jnp.concatenate([both, also], axis=0))
            product((me ^ other) * peer_blocks + q, jnp.concatenate([also, both], axis=0))
            return carry

        lax.fori_loop(0, peer_blocks, body, 0, unroll=min(8, peer_blocks))


def mix_level(me, slots, blocks, weights):
    groups, parts = len(blocks), len(weights)
    peer_blocks, rank, columns = blocks[0].shape
    return pl.pallas_call(
        functools.partial(mix_kernel, groups, parts),
        out_shape=jax.ShapeDtypeStruct((groups * peer_blocks, rank, columns), jnp.bfloat16),
        in_specs=[SMEM, SMEM] + [VMEM] * (groups + parts),
        out_specs=VMEM,
        compiler_params=pltpu.CompilerParams(vmem_limit_bytes=12 * 2**20),
        cost_estimate=cost(3),
        name="mix_level",
    )(me, slots, *blocks, *weights)


def leaf_out_kernel(sizes_ref, blocks, factor, out_hbm, out, starts, sem):
    leaves, rank, columns = blocks.shape
    points = out_hbm.shape[0]
    place_starts(sizes_ref, starts)
    sign = sign_row(rank, columns).astype(jnp.bfloat16)
    fill = jnp.zeros((TILE - 2 * rank, columns), blocks.dtype)
    row = lax.broadcasted_iota(jnp.int32, (ROWS, columns), 0)

    def body(leaf, carry):
        start = starts[leaf]
        base = pl.multiple_of(start & ~(ROWS - 1), ROWS)
        block = blocks[leaf]
        stacked = jnp.concatenate([block, turned(block, sign), fill], axis=0)
        sums = jnp.dot(
            factor[pl.ds(base, LEAFMAX + ROWS), :], stacked, preferred_element_type=jnp.float32
        )
        before = out[pl.ds(base, ROWS), :].astype(jnp.float32)
        head = jnp.where(row >= start - base, sums[:ROWS], before)
        out[pl.ds(base, ROWS), :] = head.astype(out.dtype)
        rest = pl.multiple_of(base + ROWS, ROWS)
        out[pl.ds(rest, LEAFMAX), :] = sums[ROWS:].astype(out.dtype)
        return carry

    lax.fori_loop(0, leaves, body, 0, unroll=32)
    copy = pltpu.make_async_copy(out.at[pl.ds(0, points)], out_hbm, sem)
    copy.start()
    copy.wait()


def leaf_out(sizes, blocks, factor, points):
    columns = blocks.shape[-1]
    return pl.pallas_call(
        leaf_out_kernel,
        out_shape=jax.ShapeDtypeStruct((points, columns), jnp.bfloat16),
        in_specs=[SMEM, VMEM, VMEM],
        out_specs=ANY,
        scratch_shapes=[
            pltpu.VMEM((points + LEAFMAX + ROWS, columns), jnp.bfloat16),
            pltpu.SMEM((blocks.shape[0],), jnp.int32),
            pltpu.SemaphoreType.DMA,
        ],
        compiler_params=pltpu.CompilerParams(vmem_limit_bytes=12 * 2**20),
        cost_estimate=cost(4),
        name="leaf_out",
    )(sizes, blocks, factor)


def local(
    groups, parts,
    signal, col_factor, row_factor, level_factor, col_leaf_sizes, row_leaf_sizes, level_order,
):
    levels, leaves = level_order.shape[0], level_order.shape[2]
    peer_blocks = leaves // groups
    index, part = lax.axis_index("blk"), lax.axis_index("rhs")
    me = jnp.stack([index, part]).astype(jnp.int32)
    order = level_order[:, 0]

    ids = lax.iota(jnp.int32, leaves)
    hit = order[:, None, :] == ids[None, :, None]
    place = jnp.sum(jnp.where(hit, ids[None, None, :], 0), axis=2)
    slots = ((place // peer_blocks) ^ index) * peer_blocks + place % peer_blocks
    def shared(own):
        held = [own]
        for k in range(1, parts):
            held.append(lax.ppermute(own, "rhs", [(p, p ^ k) for p in range(parts)]))
        return held

    outgoing, *owns = leaf_in(
        me, col_leaf_sizes[0], order[0], signal, col_factor, level_factor, groups
    )
    weights = [shared(own) for own in owns]
    for level in range(levels):
        arrived = []
        for d in range(groups):
            block = outgoing[d * peer_blocks : (d + 1) * peer_blocks]
            if d:
                block = lax.ppermute(block, "blk", [(g, g ^ d) for g in range(groups)])
            arrived.append(block)
        if level == 1:
            arrived[1], later = lax.optimization_barrier((arrived[1], row_factor))
            flipped = flip(later)
        target = slots[level + 1] if level + 1 < levels else ids
        outgoing = mix_level(me, target, arrived, weights[level])
    return leaf_out(row_leaf_sizes[0], outgoing, flipped, signal.shape[0])


def solution(mesh):
    in_specs = (
        P("blk", "rhs"),
        P(None, "blk"),
        P(None, "blk"),
        P(None, "blk", None, "rhs", None, None),
        P("blk", None),
        P("blk", None),
        P(None, "blk", None),
    )
    body = functools.partial(local, mesh.shape["blk"], mesh.shape["rhs"])
    return jax.shard_map(
        body, mesh=mesh, in_specs=in_specs, out_specs=P("blk", "rhs"), check_vma=False
    )
```

```python
import functools

import jax
import jax.numpy as jnp
from jax import lax
from jax.experimental import pallas as pl
from jax.experimental.pallas import tpu as pltpu
from jax.sharding import PartitionSpec as P


LEAFMAX = 128
LEAF_IN_KIB = 48000
TILE = 128
ROWS = 16

SMEM = pl.BlockSpec(memory_space=pltpu.SMEM)
VMEM = pl.BlockSpec(memory_space=pltpu.VMEM)
ANY = pl.BlockSpec(memory_space=pl.ANY)
HBM = pl.BlockSpec(memory_space=pltpu.HBM)


def cost(micros):
    return pl.CostEstimate(flops=micros * 10**7, bytes_accessed=0, transcendentals=0)


def sign_row(rows, columns):
    lane = lax.broadcasted_iota(jnp.int32, (rows, columns), 1)
    return jnp.where(lane < columns // 2, -1.0, 1.0)


def turned(values, sign):
    return pltpu.roll(values, values.shape[-1] // 2, 1) * sign


def place_starts(sizes_ref, starts_ref):
    def place(b, total):
        starts_ref[b] = total
        return total + sizes_ref[b]

    lax.fori_loop(0, sizes_ref.shape[0], place, jnp.int32(0), unroll=8)


def leaf_in_kernel(
    groups, leaves_ref, signal_hbm, factor_hbm, levels_hbm, out_ref, slots_ref, *refs
):
    count = levels_hbm.shape[0]
    level_refs = refs[:count]
    sizes_ref = leaves_ref.at[count]
    starts, signal, factor, inward, arrive = refs[count:]
    inputs = [
        pltpu.make_async_copy(factor_hbm, factor, inward.at[0]),
        pltpu.make_async_copy(signal_hbm, signal, inward.at[1]),
    ]
    loads = [
        pltpu.make_async_copy(levels_hbm.at[k], level_refs[k], arrive.at[k])
        for k in range(count)
    ]
    for copy in inputs:
        copy.start()
    leaves, rank, columns = out_ref.shape
    points = signal.shape[0]
    peer_blocks = leaves // groups
    me = lax.axis_index("blk")
    place_starts(sizes_ref, starts)

    def place_slot(j, carry):
        slot = ((j // peer_blocks) ^ me) * peer_blocks + j % peer_blocks
        for level in range(1, count):
            slots_ref[level, leaves_ref[level, j]] = slot
        return carry

    lax.fori_loop(0, leaves, place_slot, 0, unroll=8)
    for copy in inputs:
        copy.wait()
    for copy in loads:
        copy.start()
    lane = lax.broadcasted_iota(jnp.int32, (ROWS, 2 * TILE), 1)
    sign = sign_row(rank, columns)

    def body(slot, carry):
        group = (slot // peer_blocks) ^ me
        leaf = leaves_ref[0, group * peer_blocks + slot % peer_blocks]
        start = starts[leaf]
        chunk = jnp.minimum(start // TILE, points // TILE - 2)
        base = pl.multiple_of(chunk * TILE, TILE)
        low = start - base
        inside = (lane >= low) & (lane < low + sizes_ref[leaf])
        keep = jnp.where(inside, 1.0, 0.0).astype(jnp.bfloat16)
        weights = factor[:, pl.ds(base, 2 * TILE)]
        weights = weights.reshape(2 * rank // ROWS, ROWS, 2 * TILE) * keep[None]
        weights = weights.reshape(2 * rank, 2 * TILE)
        sums = jnp.dot(
            weights, signal[pl.ds(base, 2 * TILE), :], preferred_element_type=jnp.float32
        )
        out_ref[slot] = (sums[:rank] + turned(sums[rank:], sign)).astype(out_ref.dtype)
        return carry

    lax.fori_loop(0, leaves, body, 0, unroll=32)
    for copy in loads:
        copy.wait()


def leaf_in(sizes, order, signal, factor, level_factor, groups):
    _, columns = signal.shape
    leaves = sizes.shape[1]
    rank = factor.shape[0] // 2
    count = level_factor.shape[0]
    level = jax.ShapeDtypeStruct(level_factor.shape[1:], level_factor.dtype)
    return pl.pallas_call(
        functools.partial(leaf_in_kernel, groups),
        out_shape=[
            jax.ShapeDtypeStruct((leaves, rank, columns), jnp.bfloat16),
            jax.ShapeDtypeStruct((count, leaves), jnp.int32),
        ]
        + [level] * count,
        in_specs=[SMEM, HBM, HBM, HBM],
        out_specs=[VMEM, SMEM] + [VMEM] * count,
        scratch_shapes=[
            pltpu.SMEM((leaves,), jnp.int32),
            pltpu.VMEM(signal.shape, signal.dtype),
            pltpu.VMEM(factor.shape, factor.dtype),
            pltpu.SemaphoreType.DMA((2,)),
            pltpu.SemaphoreType.DMA((count,)),
        ],
        compiler_params=pltpu.CompilerParams(vmem_limit_bytes=LEAF_IN_KIB * 2**10),
        cost_estimate=cost(4),
        name="leaf_in",
    )(jnp.concatenate([order[:, 0], sizes], axis=0), signal, factor, level_factor)


def flip_kernel(factor, out_ref):
    rows, points = factor.shape
    fill = jnp.zeros((TILE - rows, TILE), factor.dtype)

    def body(chunk, carry):
        base = pl.multiple_of(chunk * TILE, TILE)
        piece = jnp.concatenate([factor[:, pl.ds(base, TILE)], fill], axis=0)
        out_ref[pl.ds(base, TILE), :] = piece.T
        return carry

    lax.fori_loop(0, points // TILE, body, 0, unroll=4)
    tail = LEAFMAX + ROWS
    out_ref[pl.ds(points, tail), :] = jnp.zeros((tail, TILE), factor.dtype)


def flip(factor):
    _, points = factor.shape
    return pl.pallas_call(
        flip_kernel,
        out_shape=jax.ShapeDtypeStruct((points + LEAFMAX + ROWS, TILE), factor.dtype),
        in_specs=[VMEM],
        out_specs=VMEM,
        compiler_params=pltpu.CompilerParams(vmem_limit_bytes=8 * 2**20),
        cost_estimate=cost(4),
        name="flip",
    )(factor)


def mix_pairs(groups, pairs, blocks, weights, put):
    peer_blocks, rank, columns = blocks[0].shape
    half = groups // 2
    half_leaves = half * peer_blocks
    per_part = half_leaves // len(weights)
    me, part_me = lax.axis_index("blk"), lax.axis_index("rhs")
    sign = sign_row(rank, columns).astype(jnp.bfloat16)

    def product(block, stacked):
        h, i = block // half_leaves, block % half_leaves
        source = (i // per_part) ^ part_me
        inner = i % per_part
        own = weights[0][0, h, inner]
        for k in range(1, len(weights)):
            own = jnp.where(source == k, weights[k][0, h, inner], own)
        return jnp.dot(own, stacked, preferred_element_type=jnp.float32).astype(jnp.bfloat16)

    for k, d in enumerate(pairs):

        def body(q, carry):
            first, second = blocks[2 * k][q], blocks[2 * k + 1][q]
            both = jnp.concatenate([first, turned(first, sign)], axis=0)
            also = jnp.concatenate([second, turned(second, sign)], axis=0)
            block = (me ^ d) * peer_blocks + q
            put(2 * k, q, block, product(block, jnp.concatenate([both, also], axis=0)))
            block = (me ^ d ^ half) * peer_blocks + q
            put(2 * k + 1, q, block, product(block, jnp.concatenate([also, both], axis=0)))
            return carry

        lax.fori_loop(0, peer_blocks, body, 0, unroll=min(8, peer_blocks))


def mix_early_kernel(groups, pairs, *refs):
    blocks, weights, out_ref = refs[: 2 * len(pairs)], refs[2 * len(pairs) : -1], refs[-1]

    def put(k, q, block, value):
        out_ref[k, q] = value

    mix_pairs(groups, pairs, blocks, weights, put)


def mix_last_kernel(groups, pairs, early_pairs, target, slots_ref, *refs):
    count = len(early_pairs)
    early, blocks = refs[:count], refs[count : count + 2 * len(pairs)]
    weights, out_ref = refs[count + 2 * len(pairs) : -1], refs[-1]
    peer_blocks = blocks[0].shape[0]
    me = lax.axis_index("blk")

    def slot_of(block):
        return block if target is None else slots_ref[target, block]

    def put(k, q, block, value):
        out_ref[slot_of(block)] = value

    mix_pairs(groups, pairs, blocks, weights, put)
    for held, members in zip(early, early_pairs):
        for k, d in enumerate(e for d in members for e in (d, d ^ (groups // 2))):
            for q in range(peer_blocks):
                out_ref[slot_of((me ^ d) * peer_blocks + q)] = held[k, q]


def mix_level(level, levels, slots, blocks, weights, stages):
    groups, parts = len(blocks), len(weights)
    peer_blocks, rank, columns = blocks[0].shape
    params = pltpu.CompilerParams(vmem_limit_bytes=12 * 2**20)
    used = [[blocks[d ^ h] for d in pairs for h in (0, groups // 2)] for pairs in stages]
    early = []
    for k, pairs in enumerate(stages[:-1]):
        early.append(
            pl.pallas_call(
                functools.partial(mix_early_kernel, groups, pairs),
                out_shape=jax.ShapeDtypeStruct(
                    (2 * len(pairs), peer_blocks, rank, columns), jnp.bfloat16
                ),
                in_specs=[VMEM] * (len(used[k]) + parts),
                out_specs=VMEM,
                compiler_params=params,
                cost_estimate=cost(1),
                name="mix_early",
            )(*used[k], *weights)
        )
    return pl.pallas_call(
        functools.partial(
            mix_last_kernel, groups, stages[-1], stages[:-1],
            level + 1 if level + 1 < levels else None,
        ),
        out_shape=jax.ShapeDtypeStruct((groups * peer_blocks, rank, columns), jnp.bfloat16),
        in_specs=[SMEM] + [VMEM] * (len(early) + len(used[-1]) + parts),
        out_specs=VMEM,
        compiler_params=params,
        cost_estimate=cost(1),
        name="mix_last",
    )(slots, *early, *used[-1], *weights)


def leaf_out_kernel(sizes_ref, blocks, factor, out_hbm, out, starts, sem):
    leaves, rank, columns = blocks.shape
    points = out_hbm.shape[0]
    place_starts(sizes_ref, starts)
    sign = sign_row(rank, columns).astype(jnp.bfloat16)
    fill = jnp.zeros((TILE - 2 * rank, columns), blocks.dtype)
    row = lax.broadcasted_iota(jnp.int32, (ROWS, columns), 0)

    def body(leaf, carry):
        start = starts[leaf]
        base = pl.multiple_of(start & ~(ROWS - 1), ROWS)
        block = blocks[leaf]
        stacked = jnp.concatenate([block, turned(block, sign), fill], axis=0)
        sums = jnp.dot(
            factor[pl.ds(base, LEAFMAX + ROWS), :], stacked, preferred_element_type=jnp.float32
        )
        before = out[pl.ds(base, ROWS), :].astype(jnp.float32)
        head = jnp.where(row >= start - base, sums[:ROWS], before)
        out[pl.ds(base, ROWS), :] = head.astype(out.dtype)
        rest = pl.multiple_of(base + ROWS, ROWS)
        out[pl.ds(rest, LEAFMAX), :] = sums[ROWS:].astype(out.dtype)
        return carry

    lax.fori_loop(0, leaves, body, 0, unroll=32)
    copy = pltpu.make_async_copy(out.at[pl.ds(0, points)], out_hbm, sem)
    copy.start()
    copy.wait()


def leaf_out(sizes, blocks, factor, points):
    columns = blocks.shape[-1]
    return pl.pallas_call(
        leaf_out_kernel,
        out_shape=jax.ShapeDtypeStruct((points, columns), jnp.bfloat16),
        in_specs=[SMEM, VMEM, VMEM],
        out_specs=ANY,
        scratch_shapes=[
            pltpu.VMEM((points + LEAFMAX + ROWS, columns), jnp.bfloat16),
            pltpu.SMEM((blocks.shape[0],), jnp.int32),
            pltpu.SemaphoreType.DMA,
        ],
        compiler_params=pltpu.CompilerParams(vmem_limit_bytes=12 * 2**20),
        cost_estimate=cost(4),
        name="leaf_out",
    )(sizes, blocks, factor)


def stages_of(groups):
    half = groups // 2
    far = [k for k in range(half // 2)]
    near = [half // 2 + k for k in range(half // 2)]
    ordered = [d for pair in zip(near, far) for d in pair]
    first, second = 2 * len(ordered) // 4, 3 * len(ordered) // 4
    return tuple(ordered[:first]), tuple(ordered[first:second]), tuple(ordered[second:])


def issue_order(groups, stages):
    half = groups // 2
    pairs = [d for stage in stages for d in stage]
    middle = [d for d in pairs if d >= half // 2]
    inner = [d for d in pairs if d < half // 2]
    outward = [h for a, b in zip(middle, inner) for h in (a + half, b + half, a)]
    return outward + sorted(d for d in inner if d)


def local(
    groups, parts,
    signal, col_factor, row_factor, level_factor, col_leaf_sizes, row_leaf_sizes, level_order,
):
    levels, leaves = level_order.shape[0], level_order.shape[2]
    peer_blocks = leaves // groups
    stages = stages_of(groups)
    hops = issue_order(groups, stages)

    def shared(own):
        held = [own]
        for k in range(1, parts):
            held.append(lax.ppermute(own, "rhs", [(p, p ^ k) for p in range(parts)]))
        return held

    outgoing, slots, *owns = leaf_in(
        col_leaf_sizes, level_order, signal, col_factor, level_factor, groups
    )
    weights = [shared(own) for own in owns]
    flipped = flip(row_factor)
    for level in range(levels):
        arrived = [outgoing[d * peer_blocks : (d + 1) * peer_blocks] for d in range(groups)]
        for d in hops:
            arrived[d] = lax.ppermute(
                arrived[d], "blk", [(g, g ^ d) for g in range(groups)]
            )
        outgoing = mix_level(level, levels, slots, arrived, weights[level], stages)
    return leaf_out(row_leaf_sizes[0], outgoing, flipped, signal.shape[0])


def solution(mesh):
    in_specs = (
        P("blk", "rhs"),
        P(None, "blk"),
        P(None, "blk"),
        P(None, "blk", None, "rhs", None, None),
        P("blk", None),
        P("blk", None),
        P(None, "blk", None),
    )
    groups, parts = mesh.shape["blk"], mesh.shape["rhs"]

    def body(*args):
        return local(groups, parts, *args)

    return jax.shard_map(
        body, mesh=mesh, in_specs=in_specs, out_specs=P("blk", "rhs"), check_vma=False
    )
```

```python
import functools

import jax
import jax.numpy as jnp
from jax import lax
from jax.experimental import pallas as pl
from jax.experimental.pallas import tpu as pltpu
from jax.sharding import PartitionSpec as P


LEAFMAX = 128
LEAF_IN_KIB = 50300
SPLIT_KIB = 50000
TILE = 128
ROWS = 16

SMEM = pl.BlockSpec(memory_space=pltpu.SMEM)
VMEM = pl.BlockSpec(memory_space=pltpu.VMEM)
ANY = pl.BlockSpec(memory_space=pl.ANY)
HBM = pl.BlockSpec(memory_space=pltpu.HBM)


def cost(micros):
    return pl.CostEstimate(flops=micros * 10**7, bytes_accessed=0, transcendentals=0)


def sign_row(rows, columns):
    lane = lax.broadcasted_iota(jnp.int32, (rows, columns), 1)
    return jnp.where(lane < columns // 2, -1.0, 1.0)


def turned(values, sign):
    return pltpu.roll(values, values.shape[-1] // 2, 1) * sign


def place_starts(sizes_ref, starts_ref):
    def place(b, total):
        starts_ref[b] = total
        return total + sizes_ref[b]

    lax.fori_loop(0, sizes_ref.shape[0], place, jnp.int32(0), unroll=8)


def leaf_in_kernel(
    groups, leaves_ref, signal_hbm, factor_hbm, levels_hbm, out_ref, slots_ref, *refs
):
    count = levels_hbm.shape[0]
    first_ref, dense_ref, *refs = refs
    sizes_ref = leaves_ref.at[count]
    starts, signal, factor, inward, arrive = refs
    leaves, rank, columns = out_ref.shape
    points = signal.shape[0]
    early = leaves // 4
    pieces = 8
    rows = points // pieces
    first = -(-min(points, early * LEAFMAX + 2 * TILE) // rows)

    def pulled(source, target, at, sem):
        return pltpu.make_async_copy(source.at[at], target.at[at], inward.at[sem])

    by_rows = [pulled(signal_hbm, signal, pl.ds(k * rows, rows), k) for k in range(pieces)]
    by_ranks = [
        pulled(factor_hbm, factor, pl.ds(k * ROWS, ROWS), pieces + k)
        for k in range(2 * rank // ROWS)
    ]
    inputs = [by_ranks + by_rows[:first], by_rows[first:]]
    loads = [
        pltpu.make_async_copy(levels_hbm.at[0, :, h], first_ref.at[:, h], arrive.at[h])
        for h in range(first_ref.shape[1])
    ]
    for copy in inputs[0] + inputs[1]:
        copy.start()
    peer_blocks = leaves // groups
    me = lax.axis_index("blk")
    place_starts(sizes_ref, starts)

    def place_slot(j, carry):
        slot = ((j // peer_blocks) ^ me) * peer_blocks + j % peer_blocks
        for level in range(count):
            slots_ref[level, leaves_ref[level, j]] = slot
        return carry

    lax.fori_loop(0, leaves, place_slot, 0, unroll=8)
    lane = lax.broadcasted_iota(jnp.int32, (ROWS, 2 * TILE), 1)
    sign = sign_row(rank, columns)

    def body(leaf, carry):
        start = starts[leaf]
        chunk = jnp.minimum(start // TILE, points // TILE - 2)
        base = pl.multiple_of(chunk * TILE, TILE)
        low = start - base
        inside = (lane >= low) & (lane < low + sizes_ref[leaf])
        keep = jnp.where(inside, 1.0, 0.0).astype(jnp.bfloat16)
        weights = factor[:, pl.ds(base, 2 * TILE)]
        weights = weights.reshape(2 * rank // ROWS, ROWS, 2 * TILE) * keep[None]
        weights = weights.reshape(2 * rank, 2 * TILE)
        sums = jnp.dot(
            weights, signal[pl.ds(base, 2 * TILE), :], preferred_element_type=jnp.float32
        )
        value = sums[:rank] + turned(sums[rank:], sign)
        out_ref[slots_ref[0, leaf]] = value.astype(out_ref.dtype)
        return carry

    for copy in inputs[0]:
        copy.wait()
    for copy in loads:
        copy.start()
    lax.fori_loop(0, early, body, 0, unroll=32)
    for copy in inputs[1]:
        copy.wait()
    lax.fori_loop(early, leaves, body, 0, unroll=32)
    for copy in loads:
        copy.wait()
    width = first_ref.shape[2]

    def pack(i, carry):
        low, high = first_ref[0, 0, i], first_ref[0, 1, i]
        dense_ref[i] = low[:, :TILE]
        dense_ref[width + i] = high[:, :TILE]
        dense_ref[2 * width + i] = jnp.concatenate([low[:, TILE:], high[:, TILE:]], axis=1)
        return carry

    lax.fori_loop(0, width, pack, 0, unroll=8)


def leaf_in(sizes, order, signal, factor, level_factor, groups):
    _, columns = signal.shape
    leaves = sizes.shape[1]
    rank = factor.shape[0] // 2
    count = level_factor.shape[0]
    level = jax.ShapeDtypeStruct(level_factor.shape[1:], level_factor.dtype)
    return pl.pallas_call(
        functools.partial(leaf_in_kernel, groups),
        out_shape=[
            jax.ShapeDtypeStruct((leaves, rank, columns), jnp.bfloat16),
            jax.ShapeDtypeStruct((count, leaves), jnp.int32),
            level,
            jax.ShapeDtypeStruct((3 * level.shape[2], rank, TILE), level_factor.dtype),
        ],
        in_specs=[SMEM, HBM, HBM, HBM],
        out_specs=[VMEM, SMEM, VMEM, VMEM],
        scratch_shapes=[
            pltpu.SMEM((leaves,), jnp.int32),
            pltpu.VMEM(signal.shape, signal.dtype),
            pltpu.VMEM(factor.shape, factor.dtype),
            pltpu.SemaphoreType.DMA((8 + 2 * rank // ROWS,)),
            pltpu.SemaphoreType.DMA((level.shape[1],)),
        ],
        compiler_params=pltpu.CompilerParams(vmem_limit_bytes=LEAF_IN_KIB * 2**10),
        cost_estimate=cost(4),
        name="leaf_in",
    )(jnp.concatenate([order[:, 0], sizes], axis=0), signal, factor, level_factor)


def unpack_kernel(dense, out_ref):
    width = out_ref.shape[2]

    def body(i, carry):
        rest = dense[2 * width + i]
        half = rest.shape[1] // 2
        out_ref[0, 0, i] = jnp.concatenate([dense[i], rest[:, :half]], axis=1)
        out_ref[0, 1, i] = jnp.concatenate([dense[width + i], rest[:, half:]], axis=1)
        return carry

    lax.fori_loop(0, width, body, 0, unroll=8)


def unpack(dense, shape):
    return pl.pallas_call(
        unpack_kernel,
        out_shape=jax.ShapeDtypeStruct(shape, dense.dtype),
        in_specs=[VMEM],
        out_specs=VMEM,
        compiler_params=pltpu.CompilerParams(vmem_limit_bytes=8 * 2**20),
        cost_estimate=cost(1),
        name="unpack",
    )(dense)


def split_kernel(levels_hbm, *refs):
    count = len(refs) - 1
    copies = [
        pltpu.make_async_copy(levels_hbm.at[1 + k], refs[k], refs[count].at[k])
        for k in range(count)
    ]
    for copy in copies:
        copy.start()
    for copy in copies:
        copy.wait()


def split_levels(level_factor):
    count = level_factor.shape[0] - 1
    level = jax.ShapeDtypeStruct(level_factor.shape[1:], level_factor.dtype)
    return pl.pallas_call(
        split_kernel,
        out_shape=[level] * count,
        in_specs=[HBM],
        out_specs=[VMEM] * count,
        scratch_shapes=[pltpu.SemaphoreType.DMA((count,))],
        compiler_params=pltpu.CompilerParams(vmem_limit_bytes=SPLIT_KIB * 2**10),
        cost_estimate=cost(3),
        name="split_levels",
    )(level_factor)


def flip_kernel(factor, out_ref):
    rows, points = factor.shape
    fill = jnp.zeros((TILE - rows, TILE), factor.dtype)

    def body(chunk, carry):
        base = pl.multiple_of(chunk * TILE, TILE)
        piece = jnp.concatenate([factor[:, pl.ds(base, TILE)], fill], axis=0)
        out_ref[pl.ds(base, TILE), :] = piece.T
        return carry

    lax.fori_loop(0, points // TILE, body, 0, unroll=4)
    tail = LEAFMAX + ROWS
    out_ref[pl.ds(points, tail), :] = jnp.zeros((tail, TILE), factor.dtype)


def flip(factor):
    _, points = factor.shape
    return pl.pallas_call(
        flip_kernel,
        out_shape=jax.ShapeDtypeStruct((points + LEAFMAX + ROWS, TILE), factor.dtype),
        in_specs=[VMEM],
        out_specs=VMEM,
        compiler_params=pltpu.CompilerParams(vmem_limit_bytes=8 * 2**20),
        cost_estimate=cost(4),
        name="flip",
    )(factor)


def mix_pairs(groups, pairs, blocks, weights, put):
    peer_blocks, rank, columns = blocks[0].shape
    half = groups // 2
    half_leaves = half * peer_blocks
    per_part = half_leaves // len(weights)
    me, part_me = lax.axis_index("blk"), lax.axis_index("rhs")
    sign = sign_row(rank, columns).astype(jnp.bfloat16)

    def product(block, stacked):
        h, i = block // half_leaves, block % half_leaves
        source = (i // per_part) ^ part_me
        inner = i % per_part
        own = weights[0][0, h, inner]
        for k in range(1, len(weights)):
            own = jnp.where(source == k, weights[k][0, h, inner], own)
        return jnp.dot(own, stacked, preferred_element_type=jnp.float32).astype(jnp.bfloat16)

    for k, d in enumerate(pairs):

        def body(q, carry):
            first, second = blocks[2 * k][q], blocks[2 * k + 1][q]
            both = jnp.concatenate([first, turned(first, sign)], axis=0)
            also = jnp.concatenate([second, turned(second, sign)], axis=0)
            block = (me ^ d) * peer_blocks + q
            put(2 * k, q, block, product(block, jnp.concatenate([both, also], axis=0)))
            block = (me ^ d ^ half) * peer_blocks + q
            put(2 * k + 1, q, block, product(block, jnp.concatenate([also, both], axis=0)))
            return carry

        lax.fori_loop(0, peer_blocks, body, 0, unroll=min(8, peer_blocks))


def mix_early_kernel(groups, pairs, *refs):
    blocks, weights, out_ref = refs[: 2 * len(pairs)], refs[2 * len(pairs) : -1], refs[-1]

    def put(k, q, block, value):
        out_ref[k, q] = value

    mix_pairs(groups, pairs, blocks, weights, put)


def mix_last_kernel(groups, pairs, early_pairs, target, slots_any, *refs):
    count = len(early_pairs)
    early, blocks = refs[:count], refs[count : count + 2 * len(pairs)]
    weights = refs[count + 2 * len(pairs) : -4]
    out_ref, held, slots_ref, sem = refs[-4:]
    peer_blocks = blocks[0].shape[0]
    me = lax.axis_index("blk")
    copy = pltpu.make_async_copy(slots_any, slots_ref, sem)
    copy.start()

    def put(k, q, block, value):
        held[k, q] = value

    mix_pairs(groups, pairs, blocks, weights, put)
    copy.wait()
    for values, members in zip((*early, held), (*early_pairs, pairs)):
        for k, d in enumerate(e for d in members for e in (d, d ^ (groups // 2))):
            for q in range(peer_blocks):
                out_ref[slots_ref[target, (me ^ d) * peer_blocks + q]] = values[k, q]


def leaf_stage_kernel(groups, pairs, parts, first, last, sizes_any, factor, *refs):
    blocks, weights = refs[: 2 * len(pairs)], refs[2 * len(pairs) : 2 * len(pairs) + parts]
    rest = list(refs[2 * len(pairs) + parts :])
    before = None if first else rest.pop(0)
    out_ref = rest.pop(0)
    held, sizes_ref, starts, sem = rest[:4]
    total = rest[4] if last else out_ref
    peer_blocks, rank, columns = blocks[0].shape
    me = lax.axis_index("blk")
    copy = pltpu.make_async_copy(sizes_any, sizes_ref, sem)
    copy.start()

    def put(k, q, block, value):
        held[k, q] = value

    mix_pairs(groups, pairs, blocks, weights, put)
    if first:
        total[...] = jnp.zeros_like(total)
    else:
        total[...] = before[...]
    copy.wait()
    place_starts(sizes_ref.at[0], starts)
    sign = sign_row(rank, columns).astype(jnp.bfloat16)
    fill = jnp.zeros((TILE - 2 * rank, columns), jnp.bfloat16)
    span = LEAFMAX + ROWS
    row = lax.broadcasted_iota(jnp.int32, (span, columns), 0)
    for k, d in enumerate(e for d in pairs for e in (d, d ^ (groups // 2))):
        for q in range(peer_blocks):
            leaf = (me ^ d) * peer_blocks + q
            start = starts[leaf]
            base = pl.multiple_of(start & ~(ROWS - 1), ROWS)
            low = start - base
            inside = (row >= low) & (row < low + sizes_ref[0, leaf])
            keep = jnp.where(inside, 1.0, 0.0).astype(jnp.bfloat16)
            block = held[k, q]
            stacked = jnp.concatenate([block, turned(block, sign), fill], axis=0)
            sums = jnp.dot(
                factor[pl.ds(base, span), :] * keep, stacked,
                preferred_element_type=jnp.float32,
            )
            total[pl.ds(base, span), :] += sums.astype(jnp.bfloat16)
    if last:
        copy = pltpu.make_async_copy(total.at[pl.ds(0, out_ref.shape[0])], out_ref, sem)
        copy.start()
        copy.wait()


def leaf_stages(sizes, factor, blocks, weights, stages, points):
    groups, parts = len(blocks), len(weights)
    peer_blocks, rank, columns = blocks[0].shape
    span = (factor.shape[0], columns)
    total = None
    for k, pairs in enumerate(stages):
        first, last = k == 0, k == len(stages) - 1
        used = [blocks[d ^ h] for d in pairs for h in (0, groups // 2)]
        before = [] if first else [total]
        total = pl.pallas_call(
            functools.partial(leaf_stage_kernel, groups, pairs, parts, first, last),
            out_shape=jax.ShapeDtypeStruct(
                (points, columns) if last else span, jnp.bfloat16
            ),
            in_specs=[ANY] + [VMEM] * (1 + len(used) + parts + len(before)),
            out_specs=ANY if last else VMEM,
            scratch_shapes=[
                pltpu.VMEM((len(used), peer_blocks, rank, columns), jnp.bfloat16),
                pltpu.SMEM(sizes.shape, jnp.int32),
                pltpu.SMEM((sizes.shape[1],), jnp.int32),
                pltpu.SemaphoreType.DMA,
            ]
            + ([pltpu.VMEM(span, jnp.bfloat16)] if last else []),
            compiler_params=pltpu.CompilerParams(vmem_limit_bytes=16 * 2**20),
            cost_estimate=cost(2),
            name="leaf_stage",
        )(sizes, factor, *used, *weights, *before)
    return total


def mix_level(level, slots, blocks, weights, stages):
    groups, parts = len(blocks), len(weights)
    peer_blocks, rank, columns = blocks[0].shape
    params = pltpu.CompilerParams(vmem_limit_bytes=12 * 2**20)
    used = [[blocks[d ^ h] for d in pairs for h in (0, groups // 2)] for pairs in stages]
    early = []
    for k, pairs in enumerate(stages[:-1]):
        early.append(
            pl.pallas_call(
                functools.partial(mix_early_kernel, groups, pairs),
                out_shape=jax.ShapeDtypeStruct(
                    (2 * len(pairs), peer_blocks, rank, columns), jnp.bfloat16
                ),
                in_specs=[VMEM] * (len(used[k]) + parts),
                out_specs=VMEM,
                compiler_params=params,
                cost_estimate=cost(1),
                name="mix_early",
            )(*used[k], *weights)
        )
    return pl.pallas_call(
        functools.partial(
            mix_last_kernel, groups, stages[-1], stages[:-1], level + 1
        ),
        out_shape=jax.ShapeDtypeStruct((groups * peer_blocks, rank, columns), jnp.bfloat16),
        in_specs=[ANY] + [VMEM] * (len(early) + len(used[-1]) + parts),
        out_specs=VMEM,
        scratch_shapes=[
            pltpu.VMEM((len(used[-1]), peer_blocks, rank, columns), jnp.bfloat16),
            pltpu.SMEM(slots.shape, jnp.int32),
            pltpu.SemaphoreType.DMA,
        ],
        compiler_params=params,
        cost_estimate=cost(1),
        name="mix_last",
    )(slots, *early, *used[-1], *weights)


def stages_of(groups):
    half = groups // 2
    far = [k for k in range(half // 2)]
    near = [half // 2 + k for k in range(half // 2)]
    ordered = [d for pair in zip(near, far) for d in pair]
    first, second = 2 * len(ordered) // 4, 3 * len(ordered) // 4
    return tuple(ordered[:first]), tuple(ordered[first:second]), tuple(ordered[second:])


def issue_order(groups, stages):
    half = groups // 2
    pairs = [d for stage in stages for d in stage]
    middle = [d for d in pairs if d >= half // 2]
    inner = [d for d in pairs if d < half // 2]
    outward = [h for a, b in zip(middle, inner) for h in (b + half, a + half, a)]
    return outward + sorted(d for d in inner if d)


def local(
    groups, parts,
    signal, col_factor, row_factor, level_factor, col_leaf_sizes, row_leaf_sizes, level_order,
):
    levels, leaves = level_order.shape[0], level_order.shape[2]
    peer_blocks = leaves // groups
    stages = stages_of(groups)
    hops = issue_order(groups, stages)

    def shared(own):
        return [
            lax.ppermute(own, "rhs", [(p, p ^ k) for p in range(parts)])
            for k in range(1, parts)
        ]

    outgoing, slots, own, dense = leaf_in(
        col_leaf_sizes, level_order, signal, col_factor, level_factor, groups
    )
    owns = split_levels(level_factor)
    weights = [[own] + [unpack(other, own.shape) for other in shared(dense)]]
    weights += [[own] + shared(own) for own in owns]
    flipped = flip(row_factor)
    for level in range(levels):
        arrived = [outgoing[d * peer_blocks : (d + 1) * peer_blocks] for d in range(groups)]
        for d in hops:
            arrived[d] = lax.ppermute(
                arrived[d], "blk", [(g, g ^ d) for g in range(groups)]
            )
        if level + 1 < levels:
            outgoing = mix_level(level, slots, arrived, weights[level], stages)
    return leaf_stages(row_leaf_sizes, flipped, arrived, weights[-1], stages, signal.shape[0])


def solution(mesh):
    in_specs = (
        P("blk", "rhs"),
        P(None, "blk"),
        P(None, "blk"),
        P(None, "blk", None, "rhs", None, None),
        P("blk", None),
        P("blk", None),
        P(None, "blk", None),
    )
    groups, parts = mesh.shape["blk"], mesh.shape["rhs"]

    def body(*args):
        return local(groups, parts, *args)

    return jax.shard_map(
        body, mesh=mesh, in_specs=in_specs, out_specs=P("blk", "rhs"), check_vma=False
    )
```

```python
import functools

import jax
import jax.numpy as jnp
from jax import lax
from jax.experimental import pallas as pl
from jax.experimental.pallas import tpu as pltpu
from jax.sharding import PartitionSpec as P


LEAFMAX = 128
LEAF_IN_KIB = 50300
SPLIT_KIB = 50000
TILE = 128
ROWS = 16

SMEM = pl.BlockSpec(memory_space=pltpu.SMEM)
VMEM = pl.BlockSpec(memory_space=pltpu.VMEM)
ANY = pl.BlockSpec(memory_space=pl.ANY)
HBM = pl.BlockSpec(memory_space=pltpu.HBM)


def cost(micros):
    return pl.CostEstimate(flops=micros * 10**7, bytes_accessed=0, transcendentals=0)


def sign_row(rows, columns):
    lane = lax.broadcasted_iota(jnp.int32, (rows, columns), 1)
    return jnp.where(lane < columns // 2, -1.0, 1.0)


def turned(values, sign):
    return pltpu.roll(values, values.shape[-1] // 2, 1) * sign


def place_starts(sizes_ref, starts_ref):
    def place(b, total):
        starts_ref[b] = total
        return total + sizes_ref[b]

    lax.fori_loop(0, sizes_ref.shape[0], place, jnp.int32(0), unroll=8)


def leaf_in_kernel(
    groups, leaves_ref, signal_hbm, factor_hbm, levels_hbm, out_ref, slots_ref, *refs
):
    count = levels_hbm.shape[0]
    first_ref, dense_ref, *refs = refs
    sizes_ref = leaves_ref.at[count]
    starts, signal, factor, inward, arrive = refs
    leaves, rank, columns = out_ref.shape
    points = signal.shape[0]
    early = leaves // 4
    pieces = 8
    rows = points // pieces
    first = -(-min(points, early * LEAFMAX + 2 * TILE) // rows)

    def pulled(source, target, at, sem):
        return pltpu.make_async_copy(source.at[at], target.at[at], inward.at[sem])

    by_rows = [pulled(signal_hbm, signal, pl.ds(k * rows, rows), k) for k in range(pieces)]
    by_ranks = [
        pulled(factor_hbm, factor, pl.ds(k * ROWS, ROWS), pieces + k)
        for k in range(2 * rank // ROWS)
    ]
    inputs = [by_ranks + by_rows[:first], by_rows[first:]]
    loads = [
        pltpu.make_async_copy(levels_hbm.at[0, :, h], first_ref.at[:, h], arrive.at[h])
        for h in range(first_ref.shape[1])
    ]
    for copy in inputs[0] + inputs[1]:
        copy.start()
    peer_blocks = leaves // groups
    me = lax.axis_index("blk")
    place_starts(sizes_ref, starts)

    def place_slot(j, carry):
        slot = ((j // peer_blocks) ^ me) * peer_blocks + j % peer_blocks
        for level in range(count):
            slots_ref[level, leaves_ref[level, j]] = slot
        return carry

    lax.fori_loop(0, leaves, place_slot, 0, unroll=8)
    lane = lax.broadcasted_iota(jnp.int32, (ROWS, 2 * TILE), 1)
    sign = sign_row(rank, columns)

    def body(leaf, carry):
        start = starts[leaf]
        chunk = jnp.minimum(start // TILE, points // TILE - 2)
        base = pl.multiple_of(chunk * TILE, TILE)
        low = start - base
        inside = (lane >= low) & (lane < low + sizes_ref[leaf])
        keep = jnp.where(inside, 1.0, 0.0).astype(jnp.bfloat16)
        weights = factor[:, pl.ds(base, 2 * TILE)]
        weights = weights.reshape(2 * rank // ROWS, ROWS, 2 * TILE) * keep[None]
        weights = weights.reshape(2 * rank, 2 * TILE)
        sums = jnp.dot(
            weights, signal[pl.ds(base, 2 * TILE), :], preferred_element_type=jnp.float32
        )
        value = sums[:rank] + turned(sums[rank:], sign)
        out_ref[slots_ref[0, leaf]] = value.astype(out_ref.dtype)
        return carry

    for copy in inputs[0]:
        copy.wait()
    for copy in loads:
        copy.start()
    lax.fori_loop(0, early, body, 0, unroll=32)
    for copy in inputs[1]:
        copy.wait()
    lax.fori_loop(early, leaves, body, 0, unroll=32)
    for copy in loads:
        copy.wait()
    width = first_ref.shape[2]

    def pack(i, carry):
        low, high = first_ref[0, 0, i], first_ref[0, 1, i]
        dense_ref[i] = low[:, :TILE]
        dense_ref[width + i] = high[:, :TILE]
        dense_ref[2 * width + i] = jnp.concatenate([low[:, TILE:], high[:, TILE:]], axis=1)
        return carry

    lax.fori_loop(0, width, pack, 0, unroll=8)


def leaf_in(sizes, order, signal, factor, level_factor, groups):
    _, columns = signal.shape
    leaves = sizes.shape[1]
    rank = factor.shape[0] // 2
    count = level_factor.shape[0]
    level = jax.ShapeDtypeStruct(level_factor.shape[1:], level_factor.dtype)
    return pl.pallas_call(
        functools.partial(leaf_in_kernel, groups),
        out_shape=[
            jax.ShapeDtypeStruct((leaves, rank, columns), jnp.bfloat16),
            jax.ShapeDtypeStruct((count, leaves), jnp.int32),
            level,
            jax.ShapeDtypeStruct((3 * level.shape[2], rank, TILE), level_factor.dtype),
        ],
        in_specs=[SMEM, HBM, HBM, HBM],
        out_specs=[VMEM, SMEM, VMEM, VMEM],
        scratch_shapes=[
            pltpu.SMEM((leaves,), jnp.int32),
            pltpu.VMEM(signal.shape, signal.dtype),
            pltpu.VMEM(factor.shape, factor.dtype),
            pltpu.SemaphoreType.DMA((8 + 2 * rank // ROWS,)),
            pltpu.SemaphoreType.DMA((level.shape[1],)),
        ],
        compiler_params=pltpu.CompilerParams(vmem_limit_bytes=LEAF_IN_KIB * 2**10),
        cost_estimate=cost(4),
        name="leaf_in",
    )(jnp.concatenate([order[:, 0], sizes], axis=0), signal, factor, level_factor)


def unpack_kernel(dense, out_ref):
    width = out_ref.shape[2]

    def body(i, carry):
        rest = dense[2 * width + i]
        half = rest.shape[1] // 2
        out_ref[0, 0, i] = jnp.concatenate([dense[i], rest[:, :half]], axis=1)
        out_ref[0, 1, i] = jnp.concatenate([dense[width + i], rest[:, half:]], axis=1)
        return carry

    lax.fori_loop(0, width, body, 0, unroll=8)


def unpack(dense, shape):
    return pl.pallas_call(
        unpack_kernel,
        out_shape=jax.ShapeDtypeStruct(shape, dense.dtype),
        in_specs=[VMEM],
        out_specs=VMEM,
        compiler_params=pltpu.CompilerParams(vmem_limit_bytes=8 * 2**20),
        cost_estimate=cost(1),
        name="unpack",
    )(dense)


def split_kernel(levels_hbm, *refs):
    count = len(refs) - 1
    copies = [
        pltpu.make_async_copy(levels_hbm.at[1 + k], refs[k], refs[count].at[k])
        for k in range(count)
    ]
    for copy in copies:
        copy.start()
    for copy in copies:
        copy.wait()


def split_levels(level_factor):
    count = level_factor.shape[0] - 1
    level = jax.ShapeDtypeStruct(level_factor.shape[1:], level_factor.dtype)
    return pl.pallas_call(
        split_kernel,
        out_shape=[level] * count,
        in_specs=[HBM],
        out_specs=[VMEM] * count,
        scratch_shapes=[pltpu.SemaphoreType.DMA((count,))],
        compiler_params=pltpu.CompilerParams(vmem_limit_bytes=SPLIT_KIB * 2**10),
        cost_estimate=cost(3),
        name="split_levels",
    )(level_factor)


def flip_kernel(factor, out_ref):
    rows, points = factor.shape
    fill = jnp.zeros((TILE - rows, TILE), factor.dtype)

    def body(chunk, carry):
        base = pl.multiple_of(chunk * TILE, TILE)
        piece = jnp.concatenate([factor[:, pl.ds(base, TILE)], fill], axis=0)
        out_ref[pl.ds(base, TILE), :] = piece.T
        return carry

    lax.fori_loop(0, points // TILE, body, 0, unroll=4)
    tail = LEAFMAX + ROWS
    out_ref[pl.ds(points, tail), :] = jnp.zeros((tail, TILE), factor.dtype)


def flip(factor):
    _, points = factor.shape
    return pl.pallas_call(
        flip_kernel,
        out_shape=jax.ShapeDtypeStruct((points + LEAFMAX + ROWS, TILE), factor.dtype),
        in_specs=[VMEM],
        out_specs=VMEM,
        compiler_params=pltpu.CompilerParams(vmem_limit_bytes=8 * 2**20),
        cost_estimate=cost(4),
        name="flip",
    )(factor)


def mix_pairs(groups, pairs, blocks, weights, put):
    peer_blocks, rank, columns = blocks[0].shape
    half = groups // 2
    half_leaves = half * peer_blocks
    per_part = half_leaves // len(weights)
    me, part_me = lax.axis_index("blk"), lax.axis_index("rhs")
    sign = sign_row(rank, columns).astype(jnp.bfloat16)

    def product(block, stacked):
        h, i = block // half_leaves, block % half_leaves
        source = (i // per_part) ^ part_me
        inner = i % per_part
        own = weights[0][0, h, inner]
        for k in range(1, len(weights)):
            own = jnp.where(source == k, weights[k][0, h, inner], own)
        return jnp.dot(own, stacked, preferred_element_type=jnp.float32).astype(jnp.bfloat16)

    for k, d in enumerate(pairs):

        def body(q, carry):
            first, second = blocks[2 * k][q], blocks[2 * k + 1][q]
            both = jnp.concatenate([first, turned(first, sign)], axis=0)
            also = jnp.concatenate([second, turned(second, sign)], axis=0)
            block = (me ^ d) * peer_blocks + q
            put(2 * k, q, block, product(block, jnp.concatenate([both, also], axis=0)))
            block = (me ^ d ^ half) * peer_blocks + q
            put(2 * k + 1, q, block, product(block, jnp.concatenate([also, both], axis=0)))
            return carry

        lax.fori_loop(0, peer_blocks, body, 0, unroll=min(8, peer_blocks))


def mix_early_kernel(groups, pairs, *refs):
    blocks, weights, out_ref = refs[: 2 * len(pairs)], refs[2 * len(pairs) : -1], refs[-1]

    def put(k, q, block, value):
        out_ref[k, q] = value

    mix_pairs(groups, pairs, blocks, weights, put)


def mix_place_kernel(groups, pairs, early_pairs, onto, target, slots_any, *refs):
    before, refs = (refs[0], refs[1:]) if onto else (None, refs)
    count = len(early_pairs)
    early, blocks = refs[:count], refs[count : count + 2 * len(pairs)]
    weights = refs[count + 2 * len(pairs) : -4]
    out_ref, held, slots_ref, sem = refs[-4:]
    peer_blocks = blocks[0].shape[0]
    me = lax.axis_index("blk")
    copy = pltpu.make_async_copy(slots_any, slots_ref, sem)
    copy.start()

    def put(k, q, block, value):
        held[k, q] = value

    mix_pairs(groups, pairs, blocks, weights, put)
    if onto:
        out_ref[...] = before[...]
    copy.wait()
    for values, members in zip((*early, held), (*early_pairs, pairs)):
        for k, d in enumerate(e for d in members for e in (d, d ^ (groups // 2))):
            for q in range(peer_blocks):
                out_ref[slots_ref[target, (me ^ d) * peer_blocks + q]] = values[k, q]


def leaf_stage_kernel(groups, pairs, parts, first, last, sizes_any, factor, *refs):
    blocks, weights = refs[: 2 * len(pairs)], refs[2 * len(pairs) : 2 * len(pairs) + parts]
    rest = list(refs[2 * len(pairs) + parts :])
    before = None if first else rest.pop(0)
    out_ref = rest.pop(0)
    held, sizes_ref, starts, sem = rest[:4]
    total = rest[4] if last else out_ref
    peer_blocks, rank, columns = blocks[0].shape
    me = lax.axis_index("blk")
    copy = pltpu.make_async_copy(sizes_any, sizes_ref, sem)
    copy.start()

    def put(k, q, block, value):
        held[k, q] = value

    mix_pairs(groups, pairs, blocks, weights, put)
    if first:
        total[...] = jnp.zeros_like(total)
    else:
        total[...] = before[...]
    copy.wait()
    place_starts(sizes_ref.at[0], starts)
    sign = sign_row(rank, columns).astype(jnp.bfloat16)
    fill = jnp.zeros((TILE - 2 * rank, columns), jnp.bfloat16)
    span = LEAFMAX + ROWS
    row = lax.broadcasted_iota(jnp.int32, (span, columns), 0)
    for k, d in enumerate(e for d in pairs for e in (d, d ^ (groups // 2))):
        for q in range(peer_blocks):
            leaf = (me ^ d) * peer_blocks + q
            start = starts[leaf]
            base = pl.multiple_of(start & ~(ROWS - 1), ROWS)
            low = start - base
            inside = (row >= low) & (row < low + sizes_ref[0, leaf])
            keep = jnp.where(inside, 1.0, 0.0).astype(jnp.bfloat16)
            block = held[k, q]
            stacked = jnp.concatenate([block, turned(block, sign), fill], axis=0)
            sums = jnp.dot(
                factor[pl.ds(base, span), :] * keep, stacked,
                preferred_element_type=jnp.float32,
            )
            total[pl.ds(base, span), :] += sums.astype(jnp.bfloat16)
    if last:
        copy = pltpu.make_async_copy(total.at[pl.ds(0, out_ref.shape[0])], out_ref, sem)
        copy.start()
        copy.wait()


def leaf_stages(sizes, factor, blocks, weights, stages, points):
    groups, parts = len(blocks), len(weights)
    peer_blocks, rank, columns = blocks[0].shape
    span = (factor.shape[0], columns)
    total = None
    for k, pairs in enumerate(stages):
        first, last = k == 0, k == len(stages) - 1
        used = [blocks[d ^ h] for d in pairs for h in (0, groups // 2)]
        before = [] if first else [total]
        total = pl.pallas_call(
            functools.partial(leaf_stage_kernel, groups, pairs, parts, first, last),
            out_shape=jax.ShapeDtypeStruct(
                (points, columns) if last else span, jnp.bfloat16
            ),
            in_specs=[ANY] + [VMEM] * (1 + len(used) + parts + len(before)),
            out_specs=ANY if last else VMEM,
            scratch_shapes=[
                pltpu.VMEM((len(used), peer_blocks, rank, columns), jnp.bfloat16),
                pltpu.SMEM(sizes.shape, jnp.int32),
                pltpu.SMEM((sizes.shape[1],), jnp.int32),
                pltpu.SemaphoreType.DMA,
            ]
            + ([pltpu.VMEM(span, jnp.bfloat16)] if last else []),
            compiler_params=pltpu.CompilerParams(vmem_limit_bytes=16 * 2**20),
            cost_estimate=cost(2),
            name="leaf_stage",
        )(sizes, factor, *used, *weights, *before)
    return total


def mix_level(level, slots, blocks, weights, stages):
    groups, parts = len(blocks), len(weights)
    peer_blocks, rank, columns = blocks[0].shape
    params = pltpu.CompilerParams(vmem_limit_bytes=12 * 2**20)
    used = [[blocks[d ^ h] for d in pairs for h in (0, groups // 2)] for pairs in stages]
    early = []
    for k, pairs in enumerate(stages[:-2]):
        early.append(
            pl.pallas_call(
                functools.partial(mix_early_kernel, groups, pairs),
                out_shape=jax.ShapeDtypeStruct(
                    (2 * len(pairs), peer_blocks, rank, columns), jnp.bfloat16
                ),
                in_specs=[VMEM] * (len(used[k]) + parts),
                out_specs=VMEM,
                compiler_params=params,
                cost_estimate=cost(1),
                name="mix_early",
            )(*used[k], *weights)
        )
    placed = None
    for k in (len(stages) - 2, len(stages) - 1):
        before = early if placed is None else [placed]
        members = stages[:-2] if placed is None else ()
        placed = pl.pallas_call(
            functools.partial(
                mix_place_kernel, groups, stages[k], members, placed is not None, level + 1
            ),
            out_shape=jax.ShapeDtypeStruct(
                (groups * peer_blocks, rank, columns), jnp.bfloat16
            ),
            in_specs=[ANY] + [VMEM] * (len(before) + len(used[k]) + parts),
            out_specs=VMEM,
            scratch_shapes=[
                pltpu.VMEM((len(used[k]), peer_blocks, rank, columns), jnp.bfloat16),
                pltpu.SMEM(slots.shape, jnp.int32),
                pltpu.SemaphoreType.DMA,
            ],
            compiler_params=params,
            cost_estimate=cost(1),
            name="mix_place",
        )(slots, *before, *used[k], *weights)
    return placed


def stages_of(groups):
    half = groups // 2
    far = [k for k in range(half // 2)]
    near = [half // 2 + k for k in range(half // 2)]
    ordered = [d for pair in zip(near, far) for d in pair]
    first, second = 2 * len(ordered) // 4, 3 * len(ordered) // 4
    return tuple(ordered[:first]), tuple(ordered[first:second]), tuple(ordered[second:])


def issue_order(groups, stages):
    half = groups // 2
    pairs = [d for stage in stages for d in stage]
    middle = [d for d in pairs if d >= half // 2]
    inner = [d for d in pairs if d < half // 2]
    outward = [h for a, b in zip(middle, inner) for h in (b + half, a + half, a)]
    return outward + sorted(d for d in inner if d)


def local(
    groups, parts,
    signal, col_factor, row_factor, level_factor, col_leaf_sizes, row_leaf_sizes, level_order,
):
    levels, leaves = level_order.shape[0], level_order.shape[2]
    peer_blocks = leaves // groups
    stages = stages_of(groups)
    hops = issue_order(groups, stages)

    def shared(own):
        return [
            lax.ppermute(own, "rhs", [(p, p ^ k) for p in range(parts)])
            for k in range(1, parts)
        ]

    outgoing, slots, own, dense = leaf_in(
        col_leaf_sizes, level_order, signal, col_factor, level_factor, groups
    )
    owns = split_levels(level_factor)
    weights = [[own] + [unpack(other, own.shape) for other in shared(dense)]]
    weights += [[own] + shared(own) for own in owns]
    flipped = flip(row_factor)
    for level in range(levels):
        arrived = [outgoing[d * peer_blocks : (d + 1) * peer_blocks] for d in range(groups)]
        for d in hops:
            arrived[d] = lax.ppermute(
                arrived[d], "blk", [(g, g ^ d) for g in range(groups)]
            )
        if level + 1 < levels:
            outgoing = mix_level(level, slots, arrived, weights[level], stages)
    return leaf_stages(row_leaf_sizes, flipped, arrived, weights[-1], stages, signal.shape[0])


def solution(mesh):
    in_specs = (
        P("blk", "rhs"),
        P(None, "blk"),
        P(None, "blk"),
        P(None, "blk", None, "rhs", None, None),
        P("blk", None),
        P("blk", None),
        P(None, "blk", None),
    )
    groups, parts = mesh.shape["blk"], mesh.shape["rhs"]

    def body(*args):
        return local(groups, parts, *args)

    return jax.shard_map(
        body, mesh=mesh, in_specs=in_specs, out_specs=P("blk", "rhs"), check_vma=False
    )
```
